16 devices in a mesh: heads: 4 (over z, y), model: 4 (over x, core).
Axes of the slice: x: 2, y: 2, z: 2, core: 2. Of those that a mesh axis runs over, the one named last changes fastest.
Arguments:
- hidden_in: bfloat16 [4096, 2560], P(None, 'model')
- seg_ids: int32 [4096], replicated
- positions: int32 [4096], replicated
- w_query: bfloat16 [2, 2560, 2048], P(None, 'model', 'heads')
- w_key: bfloat16 [2, 2560, 1024], P(None, 'model', 'heads')
- w_value: bfloat16 [2, 2560, 1024], P(None, 'model', 'heads')
- w_out: bfloat16 [2, 2048, 2560], P(None, 'heads', 'model')
- w_gate: bfloat16 [2, 2560, 10240], P(None, 'model', 'heads')
- w_up: bfloat16 [2, 2560, 10240], P(None, 'model', 'heads')
- w_down: bfloat16 [2, 10240, 2560], P(None, 'heads', 'model')
- norm_scales: float32 [2, 4, 2560], P(None, None, 'model')
- qk_scales: float32 [2, 2, 256], replicated
Outputs:
- output 1: bfloat16 [4096, 2560], P(None, 'model')
- output 2: bfloat16 [2, 4096, 4, 256], P(None, None, 'heads')
- output 3: bfloat16 [2, 4096, 4, 256], P(None, None, 'heads')
All inputs are finite; a program needn't handle non-finite values.
Results may differ from the reference program's by a relative error of at most 0.02.
Values are sent between devices in bfloat16 or wider.
A program may use at most 1 GiB of HBM per device.

```python
import jax
import jax.numpy as jnp
from jax import lax

TOKENS = 4096
D_MODEL = 2560
Q_HEADS = 8
KV_HEADS = 4
HEAD_DIM = 256
FFN_DIM = 10240
WINDOW = 1024
REQUESTS = 8
Q_BLOCK = 256
OUTLIERS = 8
NORM_EPS = 1e-6
GLOBAL_BASE = 1000000.0
GLOBAL_FACTOR = 8.0
LOCAL_BASE = 10000.0


def draw_requests(rng_key):
    cut_points = jnp.sort(jax.random.permutation(rng_key, TOKENS - 1)[:REQUESTS - 1] + 1).astype(jnp.int32)
    tok_index = jnp.arange(TOKENS, dtype=jnp.int32)
    seg_ids = jnp.sum((tok_index[:, None] >= cut_points[None, :]).astype(jnp.int32), axis=1)
    starts = jnp.concatenate([jnp.zeros((1,), jnp.int32), cut_points])
    positions = tok_index - starts[seg_ids]
    return seg_ids.astype(jnp.int32), positions.astype(jnp.int32)


def gauss_weight(rng_key, arr_shape, fan_in):
    return jax.random.normal(rng_key, arr_shape, jnp.float32) * (fan_in ** -0.5)


def setup_inputs(seed: int = 0) -> dict:
    rng_keys = jax.random.split(jax.random.key(seed), 16)
    seg_ids, positions = draw_requests(rng_keys[0])
    col_scale = jnp.exp(0.6 * jax.random.normal(rng_keys[1], (D_MODEL,), jnp.float32))
    hot_cols = jax.random.permutation(rng_keys[2], D_MODEL)[:OUTLIERS]
    col_scale = col_scale.at[hot_cols].set(20.0)
    hidden = jax.random.normal(rng_keys[3], (TOKENS, D_MODEL), jnp.float32) * col_scale[None, :]
    hidden = hidden * lax.rsqrt(jnp.mean(hidden * hidden))
    q_width = Q_HEADS * HEAD_DIM
    kv_width = KV_HEADS * HEAD_DIM
    out_cols = jnp.exp(0.5 * jax.random.normal(rng_keys[4], (2, 1, D_MODEL), jnp.float32))
    down_cols = jnp.exp(0.5 * jax.random.normal(rng_keys[5], (2, 1, D_MODEL), jnp.float32))
    return {
        'hidden_in': hidden.astype(jnp.bfloat16),
        'seg_ids': seg_ids,
        'positions': positions,
        'w_query': gauss_weight(rng_keys[6], (2, D_MODEL, q_width), D_MODEL).astype(jnp.bfloat16),
        'w_key': gauss_weight(rng_keys[7], (2, D_MODEL, kv_width), D_MODEL).astype(jnp.bfloat16),
        'w_value': gauss_weight(rng_keys[8], (2, D_MODEL, kv_width), D_MODEL).astype(jnp.bfloat16),
        'w_out': (gauss_weight(rng_keys[9], (2, q_width, D_MODEL), q_width) * out_cols).astype(jnp.bfloat16),
        'w_gate': gauss_weight(rng_keys[10], (2, D_MODEL, FFN_DIM), D_MODEL).astype(jnp.bfloat16),
        'w_up': gauss_weight(rng_keys[11], (2, D_MODEL, FFN_DIM), D_MODEL).astype(jnp.bfloat16),
        'w_down': (gauss_weight(rng_keys[12], (2, FFN_DIM, D_MODEL), FFN_DIM) * down_cols).astype(jnp.bfloat16),
        'norm_scales': 0.5 * jax.random.normal(rng_keys[13], (2, 4, D_MODEL), jnp.float32),
        'qk_scales': 0.5 * jax.random.normal(rng_keys[14], (2, 2, HEAD_DIM), jnp.float32),
    }


def gemma_norm(values, scale_row):
    mean_sq = jnp.mean(values * values, axis=-1, keepdims=True)
    return values * lax.rsqrt(mean_sq + NORM_EPS) * (1.0 + scale_row)


def rope_tables(positions, rope_base, pos_factor):
    exponents = jnp.arange(0, HEAD_DIM, 2).astype(jnp.float32) / HEAD_DIM
    inv_freq = rope_base ** (-exponents)
    angles = (positions.astype(jnp.float32) / pos_factor)[:, None] * inv_freq[None, :]
    return jnp.cos(angles), jnp.sin(angles)


def apply_rope(values, cos_tab, sin_tab):
    half_dim = values.shape[-1] // 2
    first_half = values[..., :half_dim]
    second_half = values[..., half_dim:]
    cos_bcast = cos_tab[:, None, :]
    sin_bcast = sin_tab[:, None, :]
    return jnp.concatenate([first_half * cos_bcast - second_half * sin_bcast, second_half * cos_bcast + first_half * sin_bcast], axis=-1)


def attend(query_heads, key_heads, value_heads, seg_ids, positions, window):
    group_size = Q_HEADS // KV_HEADS
    n_blocks = TOKENS // Q_BLOCK
    q_scale = HEAD_DIM ** -0.5
    key_f32 = key_heads.astype(jnp.float32)
    value_f32 = value_heads.astype(jnp.float32)
    q_blocks = query_heads.reshape(n_blocks, Q_BLOCK, KV_HEADS, group_size, HEAD_DIM)
    seg_blocks = seg_ids.reshape(n_blocks, Q_BLOCK)
    pos_blocks = positions.reshape(n_blocks, Q_BLOCK)

    def one_block(block_args):
        q_blk, seg_blk, pos_blk = block_args
        scores = jnp.einsum('qkgd,tkd->kgqt', q_blk.astype(jnp.float32), key_f32) * q_scale
        pos_gap = pos_blk[:, None] - positions[None, :]
        allowed = (seg_blk[:, None] == seg_ids[None, :]) & (pos_gap >= 0) & (pos_gap < window)
        scores = jnp.where(allowed[None, None], scores, -1e30)
        row_max = jnp.max(scores, axis=-1, keepdims=True)
        exp_scores = jnp.exp(scores - row_max)
        probs_bf = (exp_scores / jnp.sum(exp_scores, axis=-1, keepdims=True)).astype(jnp.bfloat16)
        blk_out = jnp.einsum('kgqt,tkd->qkgd', probs_bf.astype(jnp.float32), value_f32)
        return blk_out.astype(jnp.bfloat16)

    attn_out = lax.map(one_block, (q_blocks, seg_blocks, pos_blocks))
    return attn_out.reshape(TOKENS, Q_HEADS * HEAD_DIM)


def run_layer(hidden, seg_ids, positions, layer_w, norm_row, qk_row, rope_base, pos_factor, window):
    w_query, w_key, w_value, w_out, w_gate, w_up, w_down = layer_w
    resid_f32 = hidden.astype(jnp.float32)
    normed = gemma_norm(resid_f32, norm_row[0]).astype(jnp.bfloat16)
    query_bf = jnp.dot(normed, w_query, preferred_element_type=jnp.float32).astype(jnp.bfloat16)
    keys_bf = jnp.dot(normed, w_key, preferred_element_type=jnp.float32).astype(jnp.bfloat16)
    values_bf = jnp.dot(normed, w_value, preferred_element_type=jnp.float32).astype(jnp.bfloat16)
    cos_tab, sin_tab = rope_tables(positions, rope_base, pos_factor)
    query_heads = apply_rope(gemma_norm(query_bf.astype(jnp.float32).reshape(TOKENS, Q_HEADS, HEAD_DIM), qk_row[0]), cos_tab, sin_tab).astype(jnp.bfloat16)
    key_heads = apply_rope(gemma_norm(keys_bf.astype(jnp.float32).reshape(TOKENS, KV_HEADS, HEAD_DIM), qk_row[1]), cos_tab, sin_tab).astype(jnp.bfloat16)
    value_heads = values_bf.reshape(TOKENS, KV_HEADS, HEAD_DIM)
    attn_out = attend(query_heads, key_heads, value_heads, seg_ids, positions, window)
    attn_sum = jnp.dot(attn_out, w_out, preferred_element_type=jnp.float32).astype(jnp.bfloat16)
    hidden_mid = (resid_f32 + gemma_norm(attn_sum.astype(jnp.float32), norm_row[1])).astype(jnp.bfloat16)
    mid_f32 = hidden_mid.astype(jnp.float32)
    normed_ffn = gemma_norm(mid_f32, norm_row[2]).astype(jnp.bfloat16)
    gate_bf = jnp.dot(normed_ffn, w_gate, preferred_element_type=jnp.float32).astype(jnp.bfloat16)
    up_bf = jnp.dot(normed_ffn, w_up, preferred_element_type=jnp.float32).astype(jnp.bfloat16)
    ffn_in = (jax.nn.gelu(gate_bf.astype(jnp.float32), approximate=True) * up_bf.astype(jnp.float32)).astype(jnp.bfloat16)
    ffn_sum = jnp.dot(ffn_in, w_down, preferred_element_type=jnp.float32).astype(jnp.bfloat16)
    hidden_new = (mid_f32 + gemma_norm(ffn_sum.astype(jnp.float32), norm_row[3])).astype(jnp.bfloat16)
    return hidden_new, key_heads, value_heads


def reference(hidden_in, seg_ids, positions, w_query, w_key, w_value, w_out, w_gate, w_up, w_down, norm_scales, qk_scales):
    settings = ((GLOBAL_BASE, GLOBAL_FACTOR, TOKENS), (LOCAL_BASE, 1.0, WINDOW))
    hidden = hidden_in
    key_list = []
    value_list = []
    for layer_idx in range(2):
        rope_base, pos_factor, window = settings[layer_idx]
        layer_w = (w_query[layer_idx], w_key[layer_idx], w_value[layer_idx], w_out[layer_idx], w_gate[layer_idx], w_up[layer_idx], w_down[layer_idx])
        hidden, key_heads, value_heads = run_layer(hidden, seg_ids, positions, layer_w, norm_scales[layer_idx], qk_scales[layer_idx], rope_base, pos_factor, window)
        key_list.append(key_heads)
        value_list.append(value_heads)
    return hidden, jnp.stack(key_list), jnp.stack(value_list)
```

```python
import functools

import jax
import jax.numpy as jnp
from jax import lax
from jax.experimental import pallas as pl
from jax.experimental.pallas import tpu as pltpu
from jax.sharding import PartitionSpec as P

NORM_EPS = 1e-6
WINDOW = 1024
GLOBAL_BASE = 1000000.0
GLOBAL_FACTOR = 8.0
LOCAL_BASE = 10000.0
HEAD_DIM = 256
KEY_BLOCK = 512
Q_ROWS = 256
MASKED = -1e30


def rope_tables(positions, head_dim, rope_base, pos_factor):
    exponents = jnp.arange(0, head_dim, 2).astype(jnp.float32) / head_dim
    inv_freq = rope_base ** (-exponents)
    angles = (positions.astype(jnp.float32) / pos_factor)[:, None] * inv_freq[None, :]
    return jnp.cos(angles), jnp.sin(angles)


def norm_rows(values, scale_row):
    mean_sq = jnp.mean(values * values, axis=-1, keepdims=True)
    return values * lax.rsqrt(mean_sq + NORM_EPS) * (1.0 + scale_row)


def norm_rope(values_bf, scale_row, cos_tab, sin_tab):
    normed = norm_rows(values_bf.astype(jnp.float32), scale_row)
    half = normed.shape[-1] // 2
    first, second = normed[:, :half], normed[:, half:]
    return jnp.concatenate([first * cos_tab - second * sin_tab, second * cos_tab + first * sin_tab], axis=-1).astype(jnp.bfloat16)


def dot4(h_ref, w_refs):
    depth = w_refs[0].shape[0]
    total = None
    for j, w_ref in enumerate(w_refs):
        part = jnp.dot(h_ref[:, j * depth:(j + 1) * depth], w_ref[...], preferred_element_type=jnp.float32)
        total = part if total is None else total + part
    return total


def kv_kernel(h_ref, w0, w1, w2, w3, cos_ref, sin_ref, scale_ref, out_ref):
    acc = dot4(h_ref, (w0, w1, w2, w3)).astype(jnp.bfloat16)
    out_ref[:, :HEAD_DIM] = norm_rope(acc[:, :HEAD_DIM], scale_ref[...], cos_ref[...], sin_ref[...])
    out_ref[:, HEAD_DIM:] = acc[:, HEAD_DIM:]


def q_kernel(h_ref, w0, w1, w2, w3, cos_ref, sin_ref, scale_ref, out_ref):
    acc = dot4(h_ref, (w0, w1, w2, w3)).astype(jnp.bfloat16)
    for n in range(2):
        cols = slice(n * HEAD_DIM, (n + 1) * HEAD_DIM)
        out_ref[:, cols] = norm_rope(acc[:, cols], scale_ref[...], cos_ref[...], sin_ref[...])


def project(kernel, h_full, pieces, col_block, cos_tab, sin_tab, scale_row):
    n_tok, width = h_full.shape
    depth = pieces[0].shape[0]
    return pl.pallas_call(
        kernel,
        grid=(n_tok // Q_ROWS,),
        in_specs=[pl.BlockSpec((Q_ROWS, width), lambda i: (i, 0))]
        + [pl.BlockSpec((depth, 512), lambda i: (0, col_block))] * 4
        + [pl.BlockSpec((Q_ROWS, HEAD_DIM // 2), lambda i: (i, 0))] * 2
        + [pl.BlockSpec((1, HEAD_DIM), lambda i: (0, 0))],
        out_specs=pl.BlockSpec((Q_ROWS, 512), lambda i: (i, 0)),
        out_shape=jax.ShapeDtypeStruct((n_tok, 512), jnp.bfloat16),
        compiler_params=pltpu.CompilerParams(dimension_semantics=("arbitrary",)),
        cost_estimate=pl.CostEstimate(flops=2 * n_tok * width * 512, bytes_accessed=10_000_000, transcendentals=0),
    )(h_full, *pieces, cos_tab, sin_tab, scale_row)


def attention_kernel(bounds_ref, q_ref, k_ref, v_ref, low_ref, o_ref):
    step = pl.program_id(0)
    row_base = bounds_ref[0] + step * Q_ROWS
    first_block = bounds_ref[1 + step] // KEY_BLOCK
    last_block = (row_base + Q_ROWS + KEY_BLOCK - 1) // KEY_BLOCK
    q2 = jnp.concatenate([q_ref[:, :HEAD_DIM], q_ref[:, HEAD_DIM:]], axis=0)
    low = jnp.concatenate([low_ref[...], low_ref[...]], axis=0)
    rows = row_base + lax.broadcasted_iota(jnp.int32, (Q_ROWS, 1), 0)
    rows = jnp.concatenate([rows, rows], axis=0)
    scale = HEAD_DIM ** -0.5

    def one_block(block, carry):
        row_max, row_sum, acc = carry
        base = pl.multiple_of(block * KEY_BLOCK, KEY_BLOCK)
        k_blk = k_ref[pl.ds(base, KEY_BLOCK), :]
        v_blk = v_ref[pl.ds(base, KEY_BLOCK), :]
        scores = lax.dot_general(q2, k_blk, (((1,), (1,)), ((), ())), preferred_element_type=jnp.float32) * scale
        cols = base + lax.broadcasted_iota(jnp.int32, (1, KEY_BLOCK), 1)
        scores = jnp.where((cols >= low) & (cols <= rows), scores, MASKED)
        new_max = jnp.maximum(row_max, jnp.max(scores, axis=-1, keepdims=True))
        old = jnp.exp(row_max - new_max)
        probs = jnp.exp(scores - new_max)
        row_sum = row_sum * old + jnp.sum(probs, axis=-1, keepdims=True)
        acc = acc * old + jnp.dot(probs.astype(jnp.bfloat16), v_blk, preferred_element_type=jnp.float32)
        return new_max, row_sum, acc

    init = (jnp.full((2 * Q_ROWS, 1), 2 * MASKED, jnp.float32), jnp.zeros((2 * Q_ROWS, 1), jnp.float32),
            jnp.zeros((2 * Q_ROWS, HEAD_DIM), jnp.float32))
    row_max, row_sum, acc = lax.fori_loop(first_block, last_block, one_block, init)
    out = (acc / row_sum).astype(jnp.bfloat16)
    o_ref[:, :HEAD_DIM] = out[:Q_ROWS]
    o_ref[:, HEAD_DIM:] = out[Q_ROWS:]


def attend(q_loc, kv_all, low, bounds):
    n_q = q_loc.shape[0]
    n_tok = kv_all.shape[0]
    return pl.pallas_call(
        attention_kernel,
        grid_spec=pltpu.PrefetchScalarGridSpec(
            num_scalar_prefetch=1,
            grid=(n_q // Q_ROWS,),
            in_specs=[pl.BlockSpec((Q_ROWS, 512), lambda i, b: (i, 0)),
                      pl.BlockSpec((n_tok, HEAD_DIM), lambda i, b: (0, 0)),
                      pl.BlockSpec((n_tok, HEAD_DIM), lambda i, b: (0, 1)),
                      pl.BlockSpec((Q_ROWS, 1), lambda i, b: (i, 0))],
            out_specs=pl.BlockSpec((Q_ROWS, 512), lambda i, b: (i, 0))),
        out_shape=jax.ShapeDtypeStruct((n_q, 512), jnp.bfloat16),
        compiler_params=pltpu.CompilerParams(dimension_semantics=("arbitrary",)),
        cost_estimate=pl.CostEstimate(flops=2 * n_q * n_tok * 512, bytes_accessed=8_000_000, transcendentals=0),
    )(bounds, q_loc, kv_all, kv_all, low)


def ffn_up_kernel(h_ref, g0, g1, g2, g3, u0, u1, u2, u3, out_ref):
    def chunk(i, _):
        rows = pl.ds(pl.multiple_of(i * 256, 256), 256)
        h_rows = h_ref.at[rows, :]
        gate = dot4(h_rows, (g0, g1, g2, g3)).astype(jnp.bfloat16).astype(jnp.float32)
        up = dot4(h_rows, (u0, u1, u2, u3)).astype(jnp.bfloat16).astype(jnp.float32)
        out_ref[rows, :] = (jax.nn.gelu(gate, approximate=True) * up).astype(jnp.bfloat16)
        return 0

    lax.fori_loop(0, h_ref.shape[0] // 256, chunk, 0)


def ffn_up(h_full, gates, ups):
    n_tok, width = h_full.shape
    depth, n_cols = gates[0].shape
    block = 512
    return pl.pallas_call(
        ffn_up_kernel,
        grid=(n_cols // block,),
        in_specs=[pl.BlockSpec((n_tok, width), lambda n: (0, 0))] + [pl.BlockSpec((depth, block), lambda n: (0, n))] * 8,
        out_specs=pl.BlockSpec((n_tok, block), lambda n: (0, n)),
        out_shape=jax.ShapeDtypeStruct((n_tok, n_cols), jnp.bfloat16),
        compiler_params=pltpu.CompilerParams(dimension_semantics=("arbitrary",)),
        cost_estimate=pl.CostEstimate(flops=4 * n_tok * width * n_cols, bytes_accessed=40_000_000, transcendentals=n_tok * n_cols),
    )(h_full, *gates, *ups)


def solution(mesh):
    col_spec = P(None, 'model', 'heads')
    row_spec = P(None, 'heads', 'model')
    cache_spec = P(None, None, 'heads', None)

    def swap(value, bits):
        return lax.ppermute(value, 'model', [(i, i ^ bits) for i in range(4)])

    def gather_pieces(own):
        far = swap(own, 2)
        return (own, swap(own, 1), far, swap(far, 1))

    def body(hidden_in, seg_ids, positions, w_query, w_key, w_value, w_out, w_gate, w_up, w_down, norm_scales, qk_scales):
        n_tok, part = hidden_in.shape
        me = lax.axis_index('model')
        head = lax.axis_index('heads')
        rows_m = n_tok // 4
        rows_own = n_tok // 16

        scales_all = lax.all_gather(norm_scales, 'model')
        scales = jnp.concatenate([lax.dynamic_index_in_dim(scales_all, me ^ j, 0, keepdims=False) for j in range(4)], axis=-1)

        hidden = jnp.concatenate([
            swap(lax.dynamic_slice(hidden_in, ((me ^ j) * rows_m + head * rows_own, 0), (rows_own, part)), j) if j else
            lax.dynamic_slice(hidden_in, (me * rows_m + head * rows_own, 0), (rows_own, part))
            for j in range(4)], axis=1)

        index = jnp.arange(n_tok, dtype=jnp.int32)
        starts = index - positions
        pos_loc = lax.dynamic_slice(positions, (me * rows_m,), (rows_m,))

        w_qkv = jnp.concatenate([w_query, w_key, w_value], axis=-1)
        pieces = []
        for l in range(2):
            qkv_p = gather_pieces(w_qkv[l])
            out_x = jnp.concatenate([w_out[l], swap(w_out[l], 2)], axis=-1)
            out_h = lax.all_gather(out_x, 'heads', axis=0, tiled=True)
            out_c = swap(out_h, 1)
            pieces.append((qkv_p, out_h, out_c, gather_pieces(w_gate[l]), gather_pieces(w_up[l]), gather_pieces(w_down[l])))

        settings = ((GLOBAL_BASE, GLOBAL_FACTOR, n_tok), (LOCAL_BASE, 1.0, WINDOW))
        kv_list = []
        for l in range(2):
            rope_base, pos_factor, window = settings[l]
            qkv_p, out_h, out_c, gate_p, up_p, down_p = pieces[l]
            cos_tab, sin_tab = rope_tables(pos_loc, HEAD_DIM, rope_base, pos_factor)
            resid = hidden.astype(jnp.float32)
            normed = norm_rows(resid, scales[l, 0]).astype(jnp.bfloat16)
            h_full = lax.all_gather(normed, 'heads', axis=0, tiled=True)
            kv_loc = project(kv_kernel, h_full, qkv_p, 1, cos_tab, sin_tab, qk_scales[l, 1:2])
            kv_all = lax.all_gather(kv_loc, 'model', axis=0, tiled=True)
            q_loc = project(q_kernel, h_full, qkv_p, 0, cos_tab, sin_tab, qk_scales[l, 0:1])
            kv_list.append(kv_all)
            low_all = jnp.maximum(starts, index - (window - 1))
            low = lax.dynamic_slice(low_all, (me * rows_m,), (rows_m,))
            bounds = jnp.concatenate([(me * rows_m).astype(jnp.int32)[None], low[::Q_ROWS]])
            o_loc = attend(q_loc, kv_all, low[:, None], bounds)
            o_own = lax.all_to_all(o_loc, 'heads', split_axis=0, concat_axis=1, tiled=True)
            a_h = jnp.dot(o_own, out_h, preferred_element_type=jnp.float32).astype(jnp.bfloat16)
            a_c = jnp.dot(o_own, out_c, preferred_element_type=jnp.float32).astype(jnp.bfloat16)
            a_own = jnp.concatenate([a_h[:, :part], a_c[:, :part], a_h[:, part:], a_c[:, part:]], axis=1)
            mid = (resid + norm_rows(a_own.astype(jnp.float32), scales[l, 1])).astype(jnp.bfloat16)
            mid_f32 = mid.astype(jnp.float32)
            normed2 = norm_rows(mid_f32, scales[l, 2]).astype(jnp.bfloat16)
            h2_full = lax.all_gather(normed2, 'heads', axis=0, tiled=True)
            ffn_in = ffn_up(h2_full, gate_p, up_p)
            f_parts = [lax.psum_scatter(jnp.dot(ffn_in, w, preferred_element_type=jnp.float32), 'heads', scatter_dimension=0, tiled=True) for w in down_p]
            f_own = jnp.concatenate(f_parts, axis=1).astype(jnp.bfloat16)
            hidden = (mid_f32 + norm_rows(f_own.astype(jnp.float32), scales[l, 3])).astype(jnp.bfloat16)

        mine = [hidden[:, :part]] + [swap(hidden[:, j * part:(j + 1) * part], j) for j in range(1, 4)]
        stacked = jnp.stack(mine)
        ordered = jnp.stack([lax.dynamic_index_in_dim(stacked, me ^ j, 0, keepdims=False) for j in range(4)])
        full = lax.all_gather(ordered, 'heads', axis=1, tiled=True)
        hidden_out = full.reshape(n_tok, part)
        keys = jnp.stack([kv[:, :HEAD_DIM] for kv in kv_list])[:, :, None, :]
        values = jnp.stack([kv[:, HEAD_DIM:] for kv in kv_list])[:, :, None, :]
        return hidden_out, keys, values

    return jax.shard_map(body, mesh=mesh,
                         in_specs=(P(None, 'model'), P(), P(), col_spec, col_spec, col_spec, row_spec, col_spec, col_spec, row_spec, P(None, None, 'model'), P()),
                         out_specs=(P(None, 'model'), cache_spec, cache_spec),
                         check_vma=False)
```

```python
import jax
import jax.numpy as jnp
from jax import lax
from jax.experimental import pallas as pl
from jax.experimental.pallas import tpu as pltpu
from jax.sharding import PartitionSpec as P

NORM_EPS = 1e-6
WINDOW = 1024
GLOBAL_BASE = 1000000.0
GLOBAL_FACTOR = 8.0
LOCAL_BASE = 10000.0
HEAD_DIM = 256
KEY_BLOCK = 512
Q_ROWS = 256
MASKED = -1e30


def rope_tables(positions, head_dim, rope_base, pos_factor):
    exponents = jnp.arange(0, head_dim, 2).astype(jnp.float32) / head_dim
    inv_freq = rope_base ** (-exponents)
    angles = (positions.astype(jnp.float32) / pos_factor)[:, None] * inv_freq[None, :]
    return jnp.cos(angles), jnp.sin(angles)


def norm_rows(values, scale_row):
    mean_sq = jnp.mean(values * values, axis=-1, keepdims=True)
    return values * lax.rsqrt(mean_sq + NORM_EPS) * (1.0 + scale_row)


def norm_rope(values_bf, scale_row, cos_tab, sin_tab):
    normed = norm_rows(values_bf.astype(jnp.float32), scale_row)
    half = normed.shape[-1] // 2
    first, second = normed[:, :half], normed[:, half:]
    return jnp.concatenate([first * cos_tab - second * sin_tab, second * cos_tab + first * sin_tab], axis=-1).astype(jnp.bfloat16)


def dot4(h_ref, w_refs):
    depth = w_refs[0].shape[0]
    total = None
    for j, w_ref in enumerate(w_refs):
        part = jnp.dot(h_ref[:, j * depth:(j + 1) * depth], w_ref[...], preferred_element_type=jnp.float32)
        total = part if total is None else total + part
    return total


def kv_kernel(h_ref, w0, w1, w2, w3, cos_ref, sin_ref, scale_ref, out_ref):
    acc = dot4(h_ref, (w0, w1, w2, w3)).astype(jnp.bfloat16)
    out_ref[:, :HEAD_DIM] = norm_rope(acc[:, :HEAD_DIM], scale_ref[...], cos_ref[...], sin_ref[...])
    out_ref[:, HEAD_DIM:] = acc[:, HEAD_DIM:]


def q_kernel(h_ref, w0, w1, w2, w3, cos_ref, sin_ref, scale_ref, out_ref):
    acc = dot4(h_ref, (w0, w1, w2, w3)).astype(jnp.bfloat16)
    for n in range(2):
        cols = slice(n * HEAD_DIM, (n + 1) * HEAD_DIM)
        out_ref[:, cols] = norm_rope(acc[:, cols], scale_ref[...], cos_ref[...], sin_ref[...])


def project(kernel, h_full, pieces, col_block, cos_tab, sin_tab, scale_row):
    n_tok, width = h_full.shape
    depth = pieces[0].shape[0]
    return pl.pallas_call(
        kernel,
        grid=(n_tok // Q_ROWS,),
        in_specs=[pl.BlockSpec((Q_ROWS, width), lambda i: (i, 0))]
        + [pl.BlockSpec((depth, 512), lambda i: (0, col_block))] * 4
        + [pl.BlockSpec((Q_ROWS, HEAD_DIM // 2), lambda i: (i, 0))] * 2
        + [pl.BlockSpec((1, HEAD_DIM), lambda i: (0, 0))],
        out_specs=pl.BlockSpec((Q_ROWS, 512), lambda i: (i, 0)),
        out_shape=jax.ShapeDtypeStruct((n_tok, 512), jnp.bfloat16),
        compiler_params=pltpu.CompilerParams(dimension_semantics=("arbitrary",)),
        cost_estimate=pl.CostEstimate(flops=2 * n_tok * width * 512, bytes_accessed=10_000_000, transcendentals=0),
    )(h_full, *pieces, cos_tab, sin_tab, scale_row)


def attention_kernel(bounds_ref, q_ref, k_ref, v_ref, low_ref, o_ref):
    step = pl.program_id(0)
    row_base = bounds_ref[0] + step * Q_ROWS
    first_block = bounds_ref[1 + step] // KEY_BLOCK
    last_block = (row_base + Q_ROWS + KEY_BLOCK - 1) // KEY_BLOCK
    q2 = jnp.concatenate([q_ref[:, :HEAD_DIM], q_ref[:, HEAD_DIM:]], axis=0)
    low = jnp.concatenate([low_ref[...], low_ref[...]], axis=0)
    rows = row_base + lax.broadcasted_iota(jnp.int32, (Q_ROWS, 1), 0)
    rows = jnp.concatenate([rows, rows], axis=0)
    scale = HEAD_DIM ** -0.5

    def one_block(block, carry):
        row_max, row_sum, acc = carry
        base = pl.multiple_of(block * KEY_BLOCK, KEY_BLOCK)
        k_blk = k_ref[pl.ds(base, KEY_BLOCK), :]
        v_blk = v_ref[pl.ds(base, KEY_BLOCK), :]
        scores = lax.dot_general(q2, k_blk, (((1,), (1,)), ((), ())), preferred_element_type=jnp.float32) * scale
        cols = base + lax.broadcasted_iota(jnp.int32, (1, KEY_BLOCK), 1)
        scores = jnp.where((cols >= low) & (cols <= rows), scores, MASKED)
        new_max = jnp.maximum(row_max, jnp.max(scores, axis=-1, keepdims=True))
        old = jnp.exp(row_max - new_max)
        probs = jnp.exp(scores - new_max)
        row_sum = row_sum * old + jnp.sum(probs, axis=-1, keepdims=True)
        acc = acc * old + jnp.dot(probs.astype(jnp.bfloat16), v_blk, preferred_element_type=jnp.float32)
        return new_max, row_sum, acc

    init = (jnp.full((2 * Q_ROWS, 1), 2 * MASKED, jnp.float32), jnp.zeros((2 * Q_ROWS, 1), jnp.float32),
            jnp.zeros((2 * Q_ROWS, HEAD_DIM), jnp.float32))
    _, row_sum, acc = lax.fori_loop(first_block, last_block, one_block, init)
    out = (acc / row_sum).astype(jnp.bfloat16)
    o_ref[:, :HEAD_DIM] = out[:Q_ROWS]
    o_ref[:, HEAD_DIM:] = out[Q_ROWS:]


def attend(q_loc, kv_all, low, bounds):
    n_q = q_loc.shape[0]
    n_tok = kv_all.shape[0]
    return pl.pallas_call(
        attention_kernel,
        grid_spec=pltpu.PrefetchScalarGridSpec(
            num_scalar_prefetch=1,
            grid=(n_q // Q_ROWS,),
            in_specs=[pl.BlockSpec((Q_ROWS, 512), lambda i, b: (i, 0)),
                      pl.BlockSpec((n_tok, HEAD_DIM), lambda i, b: (0, 0)),
                      pl.BlockSpec((n_tok, HEAD_DIM), lambda i, b: (0, 1)),
                      pl.BlockSpec((Q_ROWS, 1), lambda i, b: (i, 0))],
            out_specs=pl.BlockSpec((Q_ROWS, 512), lambda i, b: (i, 0))),
        out_shape=jax.ShapeDtypeStruct((n_q, 512), jnp.bfloat16),
        compiler_params=pltpu.CompilerParams(dimension_semantics=("arbitrary",)),
        cost_estimate=pl.CostEstimate(flops=2 * n_q * n_tok * 512, bytes_accessed=8_000_000, transcendentals=0),
    )(bounds, q_loc, kv_all, kv_all, low)


def ffn_up_kernel(h_ref, g0, g1, g2, g3, u0, u1, u2, u3, out_ref):
    def chunk(i, _):
        rows = pl.ds(pl.multiple_of(i * 256, 256), 256)
        h_rows = h_ref.at[rows, :]
        gate = dot4(h_rows, (g0, g1, g2, g3)).astype(jnp.bfloat16).astype(jnp.float32)
        up = dot4(h_rows, (u0, u1, u2, u3)).astype(jnp.bfloat16).astype(jnp.float32)
        out_ref[rows, :] = (jax.nn.gelu(gate, approximate=True) * up).astype(jnp.bfloat16)
        return 0

    lax.fori_loop(0, h_ref.shape[0] // 256, chunk, 0)


def ffn_up(h_full, gates, ups):
    n_tok, width = h_full.shape
    depth, n_cols = gates[0].shape
    block = 512
    return pl.pallas_call(
        ffn_up_kernel,
        grid=(n_cols // block,),
        in_specs=[pl.BlockSpec((n_tok, width), lambda n: (0, 0))] + [pl.BlockSpec((depth, block), lambda n: (0, n))] * 8,
        out_specs=pl.BlockSpec((n_tok, block), lambda n: (0, n)),
        out_shape=jax.ShapeDtypeStruct((n_tok, n_cols), jnp.bfloat16),
        compiler_params=pltpu.CompilerParams(dimension_semantics=("arbitrary",)),
        cost_estimate=pl.CostEstimate(flops=4 * n_tok * width * n_cols, bytes_accessed=40_000_000, transcendentals=n_tok * n_cols),
    )(h_full, *gates, *ups)


def pre_kernel(x0, x1, x2, x3, scale_ref, hidden_ref, h_ref):
    hidden = jnp.concatenate([x0[...], x1[...], x2[...], x3[...]], axis=1)
    hidden_ref[...] = hidden
    h_ref[...] = norm_rows(hidden.astype(jnp.float32), scale_ref[...]).astype(jnp.bfloat16)


def out_kernel(o0, o1, o2, o3, a0, a1, a2, a3, b0, b1, b2, b3, resid_ref, post_ref, next_ref, mid_ref, h2_ref):
    half = a0.shape[1] // 2
    near, far = None, None
    for o, a, b in zip((o0, o1, o2, o3), (a0, a1, a2, a3), (b0, b1, b2, b3)):
        part_a = jnp.dot(o[...], a[...], preferred_element_type=jnp.float32)
        part_b = jnp.dot(o[...], b[...], preferred_element_type=jnp.float32)
        near = part_a if near is None else near + part_a
        far = part_b if far is None else far + part_b
    attn = jnp.concatenate([near[:, :half], far[:, :half], near[:, half:], far[:, half:]], axis=1)
    attn = attn.astype(jnp.bfloat16).astype(jnp.float32)
    mid = (resid_ref[...].astype(jnp.float32) + norm_rows(attn, post_ref[...])).astype(jnp.bfloat16)
    mid_ref[...] = mid
    h2_ref[...] = norm_rows(mid.astype(jnp.float32), next_ref[...]).astype(jnp.bfloat16)


def post_kernel(f0, f1, f2, f3, mid_ref, post_ref, next_ref, hidden_ref, h_ref):
    ffn = jnp.concatenate([f0[...], f1[...], f2[...], f3[...]], axis=1).astype(jnp.bfloat16).astype(jnp.float32)
    hidden = (mid_ref[...].astype(jnp.float32) + norm_rows(ffn, post_ref[...])).astype(jnp.bfloat16)
    hidden_ref[...] = hidden
    h_ref[...] = norm_rows(hidden.astype(jnp.float32), next_ref[...]).astype(jnp.bfloat16)


def whole(kernel, n_out, rows, width, flops, *args):
    blk = 128
    full = lambda v: pl.BlockSpec(v.shape, lambda i: (0, 0))
    tiled = lambda v: pl.BlockSpec((blk, v.shape[1]), lambda i: (i, 0))
    return pl.pallas_call(
        kernel,
        grid=(rows // blk,),
        in_specs=[tiled(v) if v.shape[0] == rows else full(v) for v in args],
        out_specs=[pl.BlockSpec((blk, width), lambda i: (i, 0))] * n_out,
        out_shape=[jax.ShapeDtypeStruct((rows, width), jnp.bfloat16)] * n_out,
        compiler_params=pltpu.CompilerParams(dimension_semantics=("arbitrary",)),
        cost_estimate=pl.CostEstimate(flops=flops, bytes_accessed=8_000_000, transcendentals=0),
    )(*args)


def solution(mesh):
    col_spec = P(None, 'model', 'heads')
    row_spec = P(None, 'heads', 'model')
    cache_spec = P(None, None, 'heads', None)

    def swap(value, bits, axis='model'):
        return lax.ppermute(value, axis, [(i, i ^ bits) for i in range(4)])

    def gather_pieces(own):
        far = swap(own, 2)
        near = swap(own, 1)
        diag = swap(far, 1)
        return (own, near, far, diag)

    def gather_out(own):
        both = jnp.concatenate([own, swap(own, 2)], axis=-1)
        y = swap(both, 1, 'heads')
        z = swap(both, 2, 'heads')
        d = swap(y, 2, 'heads')
        a = (both, y, z, d)
        b = tuple(swap(v, 1) for v in a)
        return a, b

    def layers(hidden_in, seg_ids, positions, w_query, w_key, w_value, w_out, w_gate, w_up, w_down, norm_scales, qk_scales):
        n_tok, part = hidden_in.shape
        width = part * 4
        me = lax.axis_index('model')
        head = lax.axis_index('heads')
        rows_m = n_tok // 4
        rows_own = n_tok // 16

        scales_all = lax.all_gather(norm_scales, 'model')
        scales = jnp.concatenate([lax.dynamic_index_in_dim(scales_all, me ^ j, 0, keepdims=False) for j in range(4)], axis=-1)
        row = lambda l, i: scales[l, i:i + 1]

        xs = [lax.dynamic_slice(hidden_in, ((me ^ j) * rows_m + head * rows_own, 0), (rows_own, part)) for j in range(4)]
        xs = [xs[0]] + [swap(xs[j], j) for j in range(1, 4)]

        index = jnp.arange(n_tok, dtype=jnp.int32)
        starts = index - positions
        pos_loc = lax.dynamic_slice(positions, (me * rows_m,), (rows_m,))

        w_qkv = jnp.concatenate([w_query, w_key, w_value], axis=-1)
        pieces = []
        for l in range(2):
            pieces.append((gather_pieces(w_qkv[l]), gather_out(w_out[l]),
                           gather_pieces(w_gate[l]), gather_pieces(w_up[l]), gather_pieces(w_down[l])))

        hidden, normed = whole(pre_kernel, 2, rows_own, width, 100_000_000, *xs, row(0, 0))

        settings = ((GLOBAL_BASE, GLOBAL_FACTOR, n_tok), (LOCAL_BASE, 1.0, WINDOW))
        kv_list = []
        for l in range(2):
            rope_base, pos_factor, window = settings[l]
            qkv_p, (out_a, out_b), gate_p, up_p, down_p = pieces[l]
            cos_tab, sin_tab = rope_tables(pos_loc, HEAD_DIM, rope_base, pos_factor)
            h_full = lax.all_gather(normed, 'heads', axis=0, tiled=True)
            kv_loc = project(kv_kernel, h_full, qkv_p, 1, cos_tab, sin_tab, qk_scales[l, 1:2])
            kv_all = lax.all_gather(kv_loc, 'model', axis=0, tiled=True)
            q_loc = project(q_kernel, h_full, qkv_p, 0, cos_tab, sin_tab, qk_scales[l, 0:1])
            kv_list.append(kv_all)
            low_all = jnp.maximum(starts, index - (window - 1))
            low = lax.dynamic_slice(low_all, (me * rows_m,), (rows_m,))
            bounds = jnp.concatenate([(me * rows_m).astype(jnp.int32)[None], low[::Q_ROWS]])
            o_loc = attend(q_loc, kv_all, low[:, None], bounds)
            os = [lax.dynamic_slice(o_loc, ((head ^ j) * rows_own, 0), (rows_own, 512)) for j in range(4)]
            os = [os[0]] + [swap(os[j], j, 'heads') for j in range(1, 4)]
            mid, normed2 = whole(out_kernel, 2, rows_own, width, 2 * rows_own * 2048 * width, *os, *out_a, *out_b, hidden, row(l, 1), row(l, 2))
            h2_full = lax.all_gather(normed2, 'heads', axis=0, tiled=True)
            ffn_in = ffn_up(h2_full, gate_p, up_p)
            f_parts = [lax.psum_scatter(jnp.dot(ffn_in, w, preferred_element_type=jnp.float32), 'heads', scatter_dimension=0, tiled=True) for w in down_p]
            hidden, normed = whole(post_kernel, 2, rows_own, width, 100_000_000, *f_parts, mid, row(l, 3), row(1, 0))

        mine = [hidden[:, :part]] + [swap(hidden[:, j * part:(j + 1) * part], j) for j in range(1, 4)]
        stacked = jnp.stack(mine)
        ordered = jnp.stack([lax.dynamic_index_in_dim(stacked, me ^ j, 0, keepdims=False) for j in range(4)])
        full = lax.all_gather(ordered, 'heads', axis=1, tiled=True)
        hidden_out = full.reshape(n_tok, part)
        keys = jnp.stack([kv[:, :HEAD_DIM] for kv in kv_list])[:, :, None, :]
        values = jnp.stack([kv[:, HEAD_DIM:] for kv in kv_list])[:, :, None, :]
        return hidden_out, keys, values

    return jax.shard_map(layers, mesh=mesh,
                         in_specs=(P(None, 'model'), P(), P(), col_spec, col_spec, col_spec, row_spec, col_spec, col_spec, row_spec, P(None, None, 'model'), P()),
                         out_specs=(P(None, 'model'), cache_spec, cache_spec),
                         check_vma=False)
```

```python
import functools

import jax
import jax.numpy as jnp
from jax import lax
from jax.experimental import pallas as pl
from jax.experimental.pallas import tpu as pltpu
from jax.sharding import PartitionSpec as P

NORM_EPS = 1e-6
WINDOW = 1024
GLOBAL_BASE = 1000000.0
GLOBAL_FACTOR = 8.0
LOCAL_BASE = 10000.0
HEAD_DIM = 256
KEY_BLOCK = 512
Q_ROWS = 256
MASKED = -1e30


def rope_tables(positions, head_dim, rope_base, pos_factor):
    exponents = jnp.arange(0, head_dim, 2).astype(jnp.float32) / head_dim
    inv_freq = rope_base ** (-exponents)
    angles = (positions.astype(jnp.float32) / pos_factor)[:, None] * inv_freq[None, :]
    return jnp.cos(angles), jnp.sin(angles)


def norm_rows(values, scale_row):
    mean_sq = jnp.mean(values * values, axis=-1, keepdims=True)
    return values * lax.rsqrt(mean_sq + NORM_EPS) * (1.0 + scale_row)


def norm_rope(values_bf, scale_row, cos_tab, sin_tab):
    normed = norm_rows(values_bf.astype(jnp.float32), scale_row)
    half = normed.shape[-1] // 2
    first, second = normed[:, :half], normed[:, half:]
    return jnp.concatenate([first * cos_tab - second * sin_tab, second * cos_tab + first * sin_tab], axis=-1).astype(jnp.bfloat16)


def dot4(h_ref, w_refs):
    depth = w_refs[0].shape[0]
    total = None
    for j, w_ref in enumerate(w_refs):
        part = jnp.dot(h_ref[:, j * depth:(j + 1) * depth], w_ref[...], preferred_element_type=jnp.float32)
        total = part if total is None else total + part
    return total


def kv_kernel(h_ref, w0, w1, w2, w3, cos_ref, sin_ref, scale_ref, out_ref):
    acc = dot4(h_ref, (w0, w1, w2, w3)).astype(jnp.bfloat16)
    out_ref[:, :HEAD_DIM] = norm_rope(acc[:, :HEAD_DIM], scale_ref[...], cos_ref[...], sin_ref[...])
    out_ref[:, HEAD_DIM:] = acc[:, HEAD_DIM:]


def q_kernel(h_ref, w0, w1, w2, w3, cos_ref, sin_ref, scale_ref, out_ref):
    acc = dot4(h_ref, (w0, w1, w2, w3)).astype(jnp.bfloat16)
    for n in range(2):
        cols = slice(n * HEAD_DIM, (n + 1) * HEAD_DIM)
        out_ref[:, cols] = norm_rope(acc[:, cols], scale_ref[...], cos_ref[...], sin_ref[...])


def project(kernel, h_full, pieces, col_block, cos_tab, sin_tab, scale_row):
    n_tok, width = h_full.shape
    depth = pieces[0].shape[0]
    return pl.pallas_call(
        kernel,
        grid=(n_tok // Q_ROWS,),
        in_specs=[pl.BlockSpec((Q_ROWS, width), lambda i: (i, 0))]
        + [pl.BlockSpec((depth, 512), lambda i: (0, col_block))] * 4
        + [pl.BlockSpec((Q_ROWS, HEAD_DIM // 2), lambda i: (i, 0))] * 2
        + [pl.BlockSpec((1, HEAD_DIM), lambda i: (0, 0))],
        out_specs=pl.BlockSpec((Q_ROWS, 512), lambda i: (i, 0)),
        out_shape=jax.ShapeDtypeStruct((n_tok, 512), jnp.bfloat16),
        compiler_params=pltpu.CompilerParams(dimension_semantics=("arbitrary",)),
        cost_estimate=pl.CostEstimate(flops=2 * n_tok * width * 512, bytes_accessed=10_000_000, transcendentals=0),
    )(h_full, *pieces, cos_tab, sin_tab, scale_row)


def attention_kernel(bounds_ref, q_ref, k_ref, v_ref, low_ref, o_ref):
    step = pl.program_id(0)
    row_base = bounds_ref[0] + step * Q_ROWS
    first_block = bounds_ref[1 + step] // KEY_BLOCK
    last_block = (row_base + Q_ROWS + KEY_BLOCK - 1) // KEY_BLOCK
    q2 = jnp.concatenate([q_ref[:, :HEAD_DIM], q_ref[:, HEAD_DIM:]], axis=0)
    low = jnp.concatenate([low_ref[...], low_ref[...]], axis=0)
    rows = row_base + lax.broadcasted_iota(jnp.int32, (Q_ROWS, 1), 0)
    rows = jnp.concatenate([rows, rows], axis=0)
    scale = HEAD_DIM ** -0.5

    def one_block(block, carry):
        row_max, row_sum, acc = carry
        base = pl.multiple_of(block * KEY_BLOCK, KEY_BLOCK)
        k_blk = k_ref[pl.ds(base, KEY_BLOCK), :]
        v_blk = v_ref[pl.ds(base, KEY_BLOCK), :]
        scores = lax.dot_general(q2, k_blk, (((1,), (1,)), ((), ())), preferred_element_type=jnp.float32) * scale
        cols = base + lax.broadcasted_iota(jnp.int32, (1, KEY_BLOCK), 1)
        scores = jnp.where((cols >= low) & (cols <= rows), scores, MASKED)
        new_max = jnp.maximum(row_max, jnp.max(scores, axis=-1, keepdims=True))
        old = jnp.exp(row_max - new_max)
        probs = jnp.exp(scores - new_max)
        row_sum = row_sum * old + jnp.sum(probs, axis=-1, keepdims=True)
        acc = acc * old + jnp.dot(probs.astype(jnp.bfloat16), v_blk, preferred_element_type=jnp.float32)
        return new_max, row_sum, acc

    init = (jnp.full((2 * Q_ROWS, 1), 2 * MASKED, jnp.float32), jnp.zeros((2 * Q_ROWS, 1), jnp.float32),
            jnp.zeros((2 * Q_ROWS, HEAD_DIM), jnp.float32))
    _, row_sum, acc = lax.fori_loop(first_block, last_block, one_block, init)
    out = (acc / row_sum).astype(jnp.bfloat16)
    o_ref[:, :HEAD_DIM] = out[:Q_ROWS]
    o_ref[:, HEAD_DIM:] = out[Q_ROWS:]


def attend(q_loc, kv_all, low, bounds):
    n_q = q_loc.shape[0]
    n_tok = kv_all.shape[0]
    return pl.pallas_call(
        attention_kernel,
        grid_spec=pltpu.PrefetchScalarGridSpec(
            num_scalar_prefetch=1,
            grid=(n_q // Q_ROWS,),
            in_specs=[pl.BlockSpec((Q_ROWS, 512), lambda i, b: (i, 0)),
                      pl.BlockSpec((n_tok, HEAD_DIM), lambda i, b: (0, 0)),
                      pl.BlockSpec((n_tok, HEAD_DIM), lambda i, b: (0, 1)),
                      pl.BlockSpec((Q_ROWS, 1), lambda i, b: (i, 0))],
            out_specs=pl.BlockSpec((Q_ROWS, 512), lambda i, b: (i, 0))),
        out_shape=jax.ShapeDtypeStruct((n_q, 512), jnp.bfloat16),
        compiler_params=pltpu.CompilerParams(dimension_semantics=("arbitrary",)),
        cost_estimate=pl.CostEstimate(flops=2 * n_q * n_tok * 512, bytes_accessed=8_000_000, transcendentals=0),
    )(bounds, q_loc, kv_all, kv_all, low)


FFN_ROWS = 256
FFN_COLS = 512


def ffn_kernel(make_next, h_ref, g0, g1, g2, g3, u0, u1, u2, u3, d0, d1, d2, d3, mid_ref, post_ref, next_ref, hidden_ref, hnext_ref,
               wg, wu, wd, h_buf, m_buf, send, own, recv, load_sem, wd_sem, h_sem, io_sem, send_sem, recv_sem):
    head = lax.axis_index('heads')
    y_pos, z_pos = head % 2, head // 2
    over_y = head + 1 - 2 * y_pos
    over_z = head + 2 - 4 * z_pos
    diag = over_y + 2 - 4 * z_pos
    chunks = (diag, over_y, over_z, head)
    depth = g0.shape[0]
    width = wg.shape[0]
    half = width // 2
    n_blocks = width // FFN_COLS

    def load_h(c):
        rows = pl.ds(pl.multiple_of(chunks[c] * FFN_ROWS, FFN_ROWS), FFN_ROWS)
        return pltpu.make_async_copy(h_ref.at[rows, :], h_buf.at[c % 2], h_sem.at[c % 2])

    def load_up(n):
        copies = []
        for j, (g, u) in enumerate(((g0, u0), (g1, u1), (g2, u2), (g3, u3))):
            cols = pl.ds(n * FFN_COLS, FFN_COLS)
            rows = pl.ds(j * depth, depth)
            copies.append(pltpu.make_async_copy(g.at[:, cols], wg.at[rows, cols], load_sem.at[n, j]))
            copies.append(pltpu.make_async_copy(u.at[:, cols], wu.at[rows, cols], load_sem.at[n, 4 + j]))
        return copies

    load_h(0).start()
    for n in range(n_blocks):
        for copy in load_up(n):
            copy.start()
    down = [pltpu.make_async_copy(d, wd.at[:, pl.ds(j * depth, depth)], wd_sem.at[j]) for j, d in enumerate((d0, d1, d2, d3))]
    for copy in down:
        copy.start()

    barrier = pltpu.get_barrier_semaphore()
    for peer in (over_y, over_z):
        pl.semaphore_signal(barrier, inc=1, device_id={'heads': peer}, device_id_type=pl.DeviceIdType.MESH)
    pl.semaphore_wait(barrier, 2)

    def up_block(c, cols):
        h = h_buf[c % 2]
        gate = jnp.dot(h, wg[:, cols], preferred_element_type=jnp.float32).astype(jnp.bfloat16).astype(jnp.float32)
        up = jnp.dot(h, wu[:, cols], preferred_element_type=jnp.float32).astype(jnp.bfloat16).astype(jnp.float32)
        m_buf[:, cols] = (jax.nn.gelu(gate, approximate=True) * up).astype(jnp.bfloat16)

    def up_chunk(c):
        load_h(c).wait()
        if c < 3:
            load_h(c + 1).start()
        if c == 0:
            for n in range(n_blocks):
                for copy in load_up(n):
                    copy.wait()
                up_block(c, slice(n * FFN_COLS, (n + 1) * FFN_COLS))
        else:
            def step(n, _):
                up_block(c, pl.ds(pl.multiple_of(n * FFN_COLS, FFN_COLS), FFN_COLS))
                return 0

            lax.fori_loop(0, n_blocks, step, 0)

    def down_half(dst, side):
        def step(n, _):
            cols = pl.ds(pl.multiple_of(n * 256, 256), 256)
            wcols = pl.ds(pl.multiple_of(side * half + n * 256, 256), 256)
            dst[:, cols] = jnp.dot(m_buf[...], wd[:, wcols], preferred_element_type=jnp.float32)
            return 0

        lax.fori_loop(0, half // 256, step, 0)

    def move(k, peer):
        return pltpu.make_async_remote_copy(src_ref=send.at[k], dst_ref=recv.at[k], send_sem=send_sem.at[k], recv_sem=recv_sem.at[k],
                                            device_id={'heads': peer}, device_id_type=pl.DeviceIdType.MESH)

    def add_received(k, got):
        def step(i, _):
            rows = pl.ds(pl.multiple_of(i * 32, 32), 32)
            send[k, rows, :] = send[k, rows, :] + recv[got, rows, :]
            return 0

        lax.fori_loop(0, FFN_ROWS // 32, step, 0)

    sends = [move(0, over_y), move(1, over_z), move(2, over_y), move(3, over_z), move(4, over_z), move(5, over_y)]
    up_chunk(0)
    for copy in down:
        copy.wait()
    down_half(send.at[0], 0)
    sends[0].start()
    down_half(send.at[1], 1)
    sends[1].start()
    up_chunk(1)
    down_half(send.at[2], 0)
    sends[2].start()
    down_half(send.at[5], 1)
    up_chunk(2)
    down_half(send.at[3], 1)
    sends[3].start()
    down_half(send.at[4], 0)
    sends[0].wait_recv()
    add_received(4, 0)
    sends[4].start()
    sends[1].wait_recv()
    add_received(5, 1)
    sends[5].start()
    up_chunk(3)
    mid_load = pltpu.make_async_copy(mid_ref, h_buf.at[0], io_sem.at[0])
    mid_load.start()
    down_half(own.at[0], 0)
    down_half(own.at[1], 1)
    mid_load.wait()
    for k in range(2, 6):
        sends[k].wait_recv()

    def finish(i, _):
        rows = pl.ds(pl.multiple_of(i * 32, 32), 32)
        a = own[0, rows, :] + recv[2, rows, :] + recv[4, rows, :]
        b = own[1, rows, :] + recv[3, rows, :] + recv[5, rows, :]
        ffn = jnp.concatenate([a, b], axis=1).astype(jnp.bfloat16).astype(jnp.float32)
        hidden = (h_buf[0, rows, :].astype(jnp.float32) + norm_rows(ffn, post_ref[...])).astype(jnp.bfloat16)
        m_buf[rows, :] = hidden
        if make_next:
            h_buf[1, rows, :] = norm_rows(hidden.astype(jnp.float32), next_ref[...]).astype(jnp.bfloat16)
        return 0

    lax.fori_loop(0, FFN_ROWS // 32, finish, 0)
    outs = [pltpu.make_async_copy(m_buf, hidden_ref, io_sem.at[1])]
    if make_next:
        outs.append(pltpu.make_async_copy(h_buf.at[1], hnext_ref, io_sem.at[2]))
    for copy in outs:
        copy.start()
    for k in range(6):
        sends[k].wait_send()
    for copy in outs:
        copy.wait()


def ffn_last_kernel(*refs):
    ffn_kernel(False, *refs[:17], None, *refs[17:])


def ffn(h_full, gates, ups, downs, mid, post, nxt, layer):
    n_tok, width = h_full.shape
    rows = mid.shape[0]
    hbm = pl.BlockSpec(memory_space=pl.ANY)
    vmem = pl.BlockSpec(memory_space=pltpu.VMEM)
    n_out = 2 if layer == 0 else 1
    return pl.pallas_call(
        functools.partial(ffn_kernel, True) if layer == 0 else ffn_last_kernel,
        in_specs=[hbm] * 14 + [vmem] * 2,
        out_specs=[hbm] * n_out,
        out_shape=[jax.ShapeDtypeStruct((rows, width), jnp.bfloat16)] * n_out,
        scratch_shapes=[pltpu.VMEM((width, width), jnp.bfloat16)] * 3
        + [pltpu.VMEM((2, FFN_ROWS, width), jnp.bfloat16), pltpu.VMEM((FFN_ROWS, width), jnp.bfloat16),
           pltpu.VMEM((6, FFN_ROWS, width // 2), jnp.float32), pltpu.VMEM((2, FFN_ROWS, width // 2), jnp.float32),
           pltpu.VMEM((6, FFN_ROWS, width // 2), jnp.float32),
           pltpu.SemaphoreType.DMA((width // FFN_COLS, 8)), pltpu.SemaphoreType.DMA((4,)), pltpu.SemaphoreType.DMA((2,)),
           pltpu.SemaphoreType.DMA((3,)), pltpu.SemaphoreType.DMA((6,)), pltpu.SemaphoreType.DMA((6,))],
        compiler_params=pltpu.CompilerParams(collective_id=layer, has_side_effects=True, vmem_limit_bytes=67043328),
        cost_estimate=pl.CostEstimate(flops=6 * n_tok * width * width, bytes_accessed=50_000_000, transcendentals=n_tok * width),
    )(h_full, *gates, *ups, *downs, mid, post, nxt)


def pre_kernel(x0, x1, x2, x3, scale_ref, hidden_ref, h_ref):
    hidden = jnp.concatenate([x0[...], x1[...], x2[...], x3[...]], axis=1)
    hidden_ref[...] = hidden
    h_ref[...] = norm_rows(hidden.astype(jnp.float32), scale_ref[...]).astype(jnp.bfloat16)


def out_kernel(o0, o1, o2, o3, a0, a1, a2, a3, a4, b0, b1, b2, b3, b4, resid_ref, post_ref, next_ref, mid_ref, h2_ref):
    half = a0.shape[1] // 2
    depth = o3.shape[1] // 2
    near, far = None, None
    for o, a, b in zip((o0[...], o1[...], o2[...], o3[:, :depth], o3[:, depth:]), (a0, a1, a2, a3, a4), (b0, b1, b2, b3, b4)):
        part_a = jnp.dot(o, a[...], preferred_element_type=jnp.float32)
        part_b = jnp.dot(o, b[...], preferred_element_type=jnp.float32)
        near = part_a if near is None else near + part_a
        far = part_b if far is None else far + part_b
    attn = jnp.concatenate([near[:, :half], far[:, :half], near[:, half:], far[:, half:]], axis=1)
    attn = attn.astype(jnp.bfloat16).astype(jnp.float32)
    mid = (resid_ref[...].astype(jnp.float32) + norm_rows(attn, post_ref[...])).astype(jnp.bfloat16)
    mid_ref[...] = mid
    h2_ref[...] = norm_rows(mid.astype(jnp.float32), next_ref[...]).astype(jnp.bfloat16)


def whole(kernel, n_out, rows, width, flops, fixed, *args):
    blk = 128
    full = lambda v: pl.BlockSpec(v.shape, lambda i: (0, 0))
    tiled = lambda v: pl.BlockSpec((blk, v.shape[1]), lambda i: (i, 0))
    return pl.pallas_call(
        kernel,
        grid=(rows // blk,),
        in_specs=[tiled(v) if v.shape[0] == rows and k not in fixed else full(v) for k, v in enumerate(args)],
        out_specs=[pl.BlockSpec((blk, width), lambda i: (i, 0))] * n_out,
        out_shape=[jax.ShapeDtypeStruct((rows, width), jnp.bfloat16)] * n_out,
        compiler_params=pltpu.CompilerParams(dimension_semantics=("arbitrary",)),
        cost_estimate=pl.CostEstimate(flops=flops, bytes_accessed=8_000_000, transcendentals=0),
    )(*args)


def solution(mesh):
    col_spec = P(None, 'model', 'heads')
    row_spec = P(None, 'heads', 'model')
    cache_spec = P(None, None, 'heads', None)

    def swap(value, bits, axis='model'):
        return lax.ppermute(value, axis, [(i, i ^ bits) for i in range(4)])

    def gather_pieces(own):
        far = swap(own, 2)
        near = swap(own, 1)
        diag = swap(far, 1)
        return (own, near, far, diag)

    def gather_out(own):
        both = jnp.concatenate([own, swap(own, 2)], axis=-1)
        y = swap(both, 1, 'heads')
        z = swap(both, 2, 'heads')
        half = both.shape[0] // 2
        d0 = swap(y[:half], 2, 'heads')
        d1 = swap(z[half:], 1, 'heads')
        a = (both, y, z, d0, d1)
        b = tuple(swap(v, 1) for v in a)
        return a, b

    def layers(hidden_in, seg_ids, positions, w_query, w_key, w_value, w_out, w_gate, w_up, w_down, norm_scales, qk_scales):
        n_tok, part = hidden_in.shape
        width = part * 4
        me = lax.axis_index('model')
        head = lax.axis_index('heads')
        rows_m = n_tok // 4
        rows_own = n_tok // 16

        scales = jnp.concatenate([norm_scales] + [swap(norm_scales, j) for j in range(1, 4)], axis=-1)
        row = lambda l, i: scales[l, i:i + 1]

        xs = [lax.dynamic_slice(hidden_in, ((me ^ j) * rows_m + head * rows_own, 0), (rows_own, part)) for j in range(4)]
        xs = [xs[0]] + [swap(xs[j], j) for j in range(1, 4)]

        index = jnp.arange(n_tok, dtype=jnp.int32)
        starts = index - positions
        pos_loc = lax.dynamic_slice(positions, (me * rows_m,), (rows_m,))

        w_qkv = jnp.concatenate([w_query, w_key, w_value], axis=-1)
        pieces = []
        for l in range(2):
            pieces.append((gather_pieces(w_qkv[l]), gather_out(w_out[l]),
                           gather_pieces(w_gate[l]), gather_pieces(w_up[l]), gather_pieces(w_down[l])))

        hidden, normed = whole(pre_kernel, 2, rows_own, width, 100_000_000, (), *xs, row(0, 0))

        settings = ((GLOBAL_BASE, GLOBAL_FACTOR, n_tok), (LOCAL_BASE, 1.0, WINDOW))
        kv_list = []
        for l in range(2):
            rope_base, pos_factor, window = settings[l]
            qkv_p, (out_a, out_b), gate_p, up_p, down_p = pieces[l]
            cos_tab, sin_tab = rope_tables(pos_loc, HEAD_DIM, rope_base, pos_factor)
            h_full = lax.all_gather(normed, 'heads', axis=0, tiled=True)
            kv_loc = project(kv_kernel, h_full, qkv_p, 1, cos_tab, sin_tab, qk_scales[l, 1:2])
            kv_all = lax.all_gather(kv_loc, 'model', axis=0, tiled=True)
            q_loc = project(q_kernel, h_full, qkv_p, 0, cos_tab, sin_tab, qk_scales[l, 0:1])
            kv_list.append(kv_all)
            low_all = jnp.maximum(starts, index - (window - 1))
            low = lax.dynamic_slice(low_all, (me * rows_m,), (rows_m,))
            bounds = jnp.concatenate([(me * rows_m).astype(jnp.int32)[None], low[::Q_ROWS]])
            o_loc = attend(q_loc, kv_all, low[:, None], bounds)
            os = [lax.dynamic_slice(o_loc, ((head ^ j) * rows_own, 0), (rows_own, 512)) for j in range(4)]
            os = [os[0]] + [swap(os[j], j, 'heads') for j in range(1, 4)]
            mid, normed2 = whole(out_kernel, 2, rows_own, width, 2 * rows_own * 2048 * width, range(4, 14), *os, *out_a, *out_b, hidden, row(l, 1), row(l, 2))
            h2_full = lax.all_gather(normed2, 'heads', axis=0, tiled=True)
            outs = ffn(h2_full, gate_p, up_p, down_p, mid, row(l, 3), row(1, 0), l)
            hidden, normed = outs if l == 0 else (outs[0], None)

        mine = [hidden[:, :part]] + [swap(hidden[:, j * part:(j + 1) * part], j) for j in range(1, 4)]
        stacked = jnp.stack(mine)
        ordered = jnp.stack([lax.dynamic_index_in_dim(stacked, me ^ j, 0, keepdims=False) for j in range(4)])
        full = lax.all_gather(ordered, 'heads', axis=1, tiled=True)
        hidden_out = full.reshape(n_tok, part)
        keys = jnp.stack([kv[:, :HEAD_DIM] for kv in kv_list])[:, :, None, :]
        values = jnp.stack([kv[:, HEAD_DIM:] for kv in kv_list])[:, :, None, :]
        return hidden_out, keys, values

    return jax.shard_map(layers, mesh=mesh,
                         in_specs=(P(None, 'model'), P(), P(), col_spec, col_spec, col_spec, row_spec, col_spec, col_spec, row_spec, P(None, None, 'model'), P()),
                         out_specs=(P(None, 'model'), cache_spec, cache_spec),
                         check_vma=False)
```

```python
import functools

import jax
import jax.numpy as jnp
from jax import lax
from jax.experimental import pallas as pl
from jax.experimental.pallas import tpu as pltpu
from jax.sharding import PartitionSpec as P

NORM_EPS = 1e-6
WINDOW = 1024
GLOBAL_BASE = 1000000.0
GLOBAL_FACTOR = 8.0
LOCAL_BASE = 10000.0
HEAD_DIM = 256
KEY_BLOCK = 512
Q_ROWS = 256
MASKED = -1e30


def rope_tables(positions, head_dim, rope_base, pos_factor):
    exponents = jnp.arange(0, head_dim, 2).astype(jnp.float32) / head_dim
    inv_freq = rope_base ** (-exponents)
    angles = (positions.astype(jnp.float32) / pos_factor)[:, None] * inv_freq[None, :]
    return jnp.cos(angles), jnp.sin(angles)


def norm_rows(values, scale_row):
    mean_sq = jnp.mean(values * values, axis=-1, keepdims=True)
    return values * lax.rsqrt(mean_sq + NORM_EPS) * (1.0 + scale_row)


def norm_rope(values_bf, scale_row, cos_tab, sin_tab):
    normed = norm_rows(values_bf.astype(jnp.float32), scale_row)
    half = normed.shape[-1] // 2
    first, second = normed[:, :half], normed[:, half:]
    return jnp.concatenate([first * cos_tab - second * sin_tab, second * cos_tab + first * sin_tab], axis=-1).astype(jnp.bfloat16)


def dot4(h_ref, w_refs):
    depth = w_refs[0].shape[0]
    total = None
    for j, w_ref in enumerate(w_refs):
        part = jnp.dot(h_ref[:, j * depth:(j + 1) * depth], w_ref[...], preferred_element_type=jnp.float32)
        total = part if total is None else total + part
    return total


def kv_kernel(h_ref, w0, w1, w2, w3, cos_ref, sin_ref, scale_ref, out_ref):
    acc = dot4(h_ref, (w0, w1, w2, w3)).astype(jnp.bfloat16)
    out_ref[:, :HEAD_DIM] = norm_rope(acc[:, :HEAD_DIM], scale_ref[...], cos_ref[...], sin_ref[...])
    out_ref[:, HEAD_DIM:] = acc[:, HEAD_DIM:]


def q_kernel(h_ref, w0, w1, w2, w3, cos_ref, sin_ref, scale_ref, out_ref):
    acc = dot4(h_ref, (w0, w1, w2, w3)).astype(jnp.bfloat16)
    for n in range(2):
        cols = slice(n * HEAD_DIM, (n + 1) * HEAD_DIM)
        out_ref[:, cols] = norm_rope(acc[:, cols], scale_ref[...], cos_ref[...], sin_ref[...])


def project(kernel, h_full, pieces, col_block, cos_tab, sin_tab, scale_row):
    n_tok, width = h_full.shape
    depth = pieces[0].shape[0]
    return pl.pallas_call(
        kernel,
        grid=(n_tok // Q_ROWS,),
        in_specs=[pl.BlockSpec((Q_ROWS, width), lambda i: (i, 0))]
        + [pl.BlockSpec((depth, 512), lambda i: (0, col_block))] * 4
        + [pl.BlockSpec((Q_ROWS, HEAD_DIM // 2), lambda i: (i, 0))] * 2
        + [pl.BlockSpec((1, HEAD_DIM), lambda i: (0, 0))],
        out_specs=pl.BlockSpec((Q_ROWS, 512), lambda i: (i, 0)),
        out_shape=jax.ShapeDtypeStruct((n_tok, 512), jnp.bfloat16),
        compiler_params=pltpu.CompilerParams(dimension_semantics=("arbitrary",)),
        cost_estimate=pl.CostEstimate(flops=2 * n_tok * width * 512, bytes_accessed=10_000_000, transcendentals=0),
    )(h_full, *pieces, cos_tab, sin_tab, scale_row)


def attention_kernel(layer, bounds_ref, q_ref, kv0, kv1, kv2, kv3, low_ref, *rest):
    o_ref, key_ref, value_ref, kv_buf, in_sem, out_sem = rest[-6:]
    step = pl.program_id(0)
    n_loc = kv0.shape[0]

    @pl.when(step == 0)
    def _():
        copies = []
        for j, piece in enumerate((kv0, kv1, kv2, kv3)):
            rows = pl.ds(pl.multiple_of(bounds_ref[5 + j], 256), n_loc)
            copies.append(pltpu.make_async_copy(piece, kv_buf.at[rows, :], in_sem.at[j]))
        for copy in copies:
            copy.start()
        for copy in copies:
            copy.wait()
        pltpu.make_async_copy(kv_buf.at[:, pl.ds(0, HEAD_DIM)], key_ref.at[layer], out_sem.at[0]).start()
        pltpu.make_async_copy(kv_buf.at[:, pl.ds(HEAD_DIM, HEAD_DIM)], value_ref.at[layer], out_sem.at[1]).start()

    row_base = bounds_ref[0] + step * Q_ROWS
    first_block = bounds_ref[1 + step] // KEY_BLOCK
    last_block = (row_base + Q_ROWS + KEY_BLOCK - 1) // KEY_BLOCK
    q2 = jnp.concatenate([q_ref[:, :HEAD_DIM], q_ref[:, HEAD_DIM:]], axis=0)
    low = jnp.concatenate([low_ref[...], low_ref[...]], axis=0)
    rows = row_base + lax.broadcasted_iota(jnp.int32, (Q_ROWS, 1), 0)
    rows = jnp.concatenate([rows, rows], axis=0)
    scale = HEAD_DIM ** -0.5

    def one_block(block, carry):
        row_max, row_sum, acc = carry
        base = pl.multiple_of(block * KEY_BLOCK, KEY_BLOCK)
        k_blk = kv_buf[pl.ds(base, KEY_BLOCK), :HEAD_DIM]
        v_blk = kv_buf[pl.ds(base, KEY_BLOCK), HEAD_DIM:]
        scores = lax.dot_general(q2, k_blk, (((1,), (1,)), ((), ())), preferred_element_type=jnp.float32) * scale
        cols = base + lax.broadcasted_iota(jnp.int32, (1, KEY_BLOCK), 1)
        scores = jnp.where((cols >= low) & (cols <= rows), scores, MASKED)
        new_max = jnp.maximum(row_max, jnp.max(scores, axis=-1, keepdims=True))
        old = jnp.exp(row_max - new_max)
        probs = jnp.exp(scores - new_max)
        row_sum = row_sum * old + jnp.sum(probs, axis=-1, keepdims=True)
        acc = acc * old + jnp.dot(probs.astype(jnp.bfloat16), v_blk, preferred_element_type=jnp.float32)
        return new_max, row_sum, acc

    init = (jnp.full((2 * Q_ROWS, 1), 2 * MASKED, jnp.float32), jnp.zeros((2 * Q_ROWS, 1), jnp.float32),
            jnp.zeros((2 * Q_ROWS, HEAD_DIM), jnp.float32))
    _, row_sum, acc = lax.fori_loop(first_block, last_block, one_block, init)
    out = (acc / row_sum).astype(jnp.bfloat16)
    o_ref[:, :HEAD_DIM] = out[:Q_ROWS]
    o_ref[:, HEAD_DIM:] = out[Q_ROWS:]

    @pl.when(step == pl.num_programs(0) - 1)
    def _():
        pltpu.make_async_copy(kv_buf.at[:, pl.ds(0, HEAD_DIM)], key_ref.at[layer], out_sem.at[0]).wait()
        pltpu.make_async_copy(kv_buf.at[:, pl.ds(HEAD_DIM, HEAD_DIM)], value_ref.at[layer], out_sem.at[1]).wait()


def attend(q_loc, kv_pieces, low, bounds, caches, layer):
    n_q = q_loc.shape[0]
    n_tok = 4 * n_q
    hbm = pl.BlockSpec(memory_space=pl.ANY)
    cache = jax.ShapeDtypeStruct((2, n_tok, HEAD_DIM), jnp.bfloat16)
    return pl.pallas_call(
        functools.partial(attention_kernel, layer),
        grid_spec=pltpu.PrefetchScalarGridSpec(
            num_scalar_prefetch=1,
            grid=(n_q // Q_ROWS,),
            in_specs=[pl.BlockSpec((Q_ROWS, 512), lambda i, b: (i, 0))] + [hbm] * 4
            + [pl.BlockSpec((Q_ROWS, 1), lambda i, b: (i, 0))] + [hbm] * len(caches),
            out_specs=[pl.BlockSpec((Q_ROWS, 512), lambda i, b: (i, 0)), hbm, hbm],
            scratch_shapes=[pltpu.VMEM((n_tok, 512), jnp.bfloat16), pltpu.SemaphoreType.DMA((4,)), pltpu.SemaphoreType.DMA((2,))]),
        out_shape=[jax.ShapeDtypeStruct((n_q, 512), jnp.bfloat16), cache, cache],
        input_output_aliases={7: 1, 8: 2} if caches else {},
        compiler_params=pltpu.CompilerParams(dimension_semantics=("arbitrary",)),
        cost_estimate=pl.CostEstimate(flops=2 * n_q * n_tok * 512, bytes_accessed=8_000_000, transcendentals=0),
    )(bounds, q_loc, *kv_pieces, low, *caches)


MESH = pl.DeviceIdType.MESH
SPLIT = 128


def head_peers():
    head = lax.axis_index('heads')
    over_y = head + 1 - 2 * (head % 2)
    over_z = head + 2 - 4 * (head // 2)
    return head, over_y, over_z, over_y + 2 - 4 * (head // 2)


def meet(peers):
    barrier = pltpu.get_barrier_semaphore()
    for peer in peers:
        pl.semaphore_signal(barrier, inc=1, device_id=peer, device_id_type=MESH)
    pl.semaphore_wait(barrier, len(peers))


def token_rows(head, part, base=0):
    return pl.ds(pl.multiple_of(base + head * 2 * SPLIT + part * SPLIT, SPLIT), SPLIT)


class HeadGather:
    def __init__(self, src, full, local_sem, send_sem, recv_sem):
        head, over_y, over_z, _ = head_peers()
        self.local = [pltpu.make_async_copy(src.at[pl.ds(p * SPLIT, SPLIT), :], full.at[token_rows(head, p), :], local_sem.at[p]) for p in range(2)]

        def remote(a, b, k, peer):
            return pltpu.make_async_remote_copy(src_ref=a, dst_ref=b, send_sem=send_sem.at[k], recv_sem=recv_sem.at[k],
                                                device_id={'heads': peer}, device_id_type=MESH)

        mine = [(src.at[pl.ds(p * SPLIT, SPLIT), :], full.at[token_rows(head, p), :]) for p in range(2)]
        self.y = [remote(*mine[p], p, over_y) for p in range(2)]
        self.z = [remote(*mine[p], 2 + p, over_z) for p in range(2)]
        top, low = full.at[token_rows(over_y, 0), :], full.at[token_rows(over_z, 1), :]
        self.forward = [remote(top, top, 4, over_z), remote(low, low, 5, over_y)]

    def start(self, p):
        for copy in (self.y[p], self.z[p], self.local[p]):
            copy.start()

    def finish(self):
        self.y[0].wait_recv()
        self.forward[0].start()
        self.z[1].wait_recv()
        self.forward[1].start()
        self.y[1].wait_recv()
        self.z[0].wait_recv()
        for copy in self.forward:
            copy.wait_recv()
        for copy in self.y + self.z + self.forward:
            copy.wait_send()
        for copy in self.local:
            copy.wait()


GATHER_SEMS = [pltpu.SemaphoreType.DMA((2,)), pltpu.SemaphoreType.DMA((6,)), pltpu.SemaphoreType.DMA((6,))]


def pre_kernel(x0, x1, x2, x3, scale_ref, hidden_ref, full_ref, h_buf, local_sem, send_sem, recv_sem):
    _, over_y, over_z, _ = head_peers()
    meet([{'heads': over_y}, {'heads': over_z}])
    gather = HeadGather(h_buf, full_ref, local_sem, send_sem, recv_sem)
    for p in range(2):
        def step(i, _):
            rows = pl.ds(pl.multiple_of(p * SPLIT + i * 32, 32), 32)
            hidden = jnp.concatenate([x0[rows, :], x1[rows, :], x2[rows, :], x3[rows, :]], axis=1)
            hidden_ref[rows, :] = hidden
            h_buf[rows, :] = norm_rows(hidden.astype(jnp.float32), scale_ref[...]).astype(jnp.bfloat16)
            return 0

        lax.fori_loop(0, SPLIT // 32, step, 0)
        gather.start(p)
    gather.finish()


def first_norm(xs, scale):
    rows, part = xs[0].shape
    vmem = pl.BlockSpec(memory_space=pltpu.VMEM)
    return pl.pallas_call(
        pre_kernel,
        in_specs=[vmem] * 5,
        out_specs=[vmem, pl.BlockSpec(memory_space=pl.ANY)],
        out_shape=[jax.ShapeDtypeStruct((rows, 4 * part), jnp.bfloat16), jax.ShapeDtypeStruct((4 * rows, 4 * part), jnp.bfloat16)],
        scratch_shapes=[pltpu.VMEM((rows, 4 * part), jnp.bfloat16)] + GATHER_SEMS,
        compiler_params=pltpu.CompilerParams(collective_id=2, has_side_effects=True),
        cost_estimate=pl.CostEstimate(flops=500_000_000, bytes_accessed=8_000_000, transcendentals=0),
        name="pre0",
    )(*xs, scale)


def out_kernel(o_ref, a0, a1, a2, a3, a4, b0, b1, b2, b3, b4, resid_ref, post_ref, next_ref, mid_ref, full_ref,
               o_buf, w_buf, a_buf, h_buf, w_sem, o_sem, os_sem, or_sem, local_sem, send_sem, recv_sem):
    head, over_y, over_z, diag = head_peers()
    part = a0.shape[1] // 2
    dim = o_ref.shape[1]
    n_rows = 2 * SPLIT
    loads = []
    start = 0
    for k, (a, b) in enumerate(((a0, b0), (a1, b1), (a2, b2), (a3, b3), (a4, b4))):
        depth = a.shape[0]
        for i, (src, col, dst) in enumerate(((a, 0, 0), (b, 0, 1), (a, 1, 2), (b, 1, 3))):
            loads.append(pltpu.make_async_copy(src.at[:, pl.ds(col * part, part)], w_buf.at[pl.ds(start, depth), pl.ds(dst * part, part)], w_sem.at[k, i]))
        start += depth

    def rows_of(h):
        return pl.ds(pl.multiple_of(h * n_rows, n_rows), n_rows)

    own = pltpu.make_async_copy(o_ref.at[rows_of(head), :], o_buf.at[:, pl.ds(0, dim)], o_sem)
    own.start()
    for copy in loads:
        copy.start()
    meet([{'heads': over_y}, {'heads': over_z}, {'heads': diag}])
    moves = [pltpu.make_async_remote_copy(src_ref=o_ref.at[rows_of(peer), :], dst_ref=o_buf.at[:, pl.ds(j * dim, dim)], send_sem=os_sem.at[j],
                                          recv_sem=or_sem.at[j], device_id={'heads': peer}, device_id_type=MESH)
             for j, peer in ((3, diag), (1, over_y), (2, over_z))]
    for copy in moves:
        copy.start()
    own.wait()
    for copy in loads:
        copy.wait()
    for copy in moves:
        copy.wait_recv()
    gather = HeadGather(h_buf, full_ref, local_sem, send_sem, recv_sem)
    for p in range(2):
        def project_block(n, _):
            cols = pl.ds(pl.multiple_of(n * 512, 512), 512)
            a_buf[:, cols] = jnp.dot(o_buf[p * SPLIT:(p + 1) * SPLIT, :], w_buf[:, cols], preferred_element_type=jnp.float32)
            return 0

        lax.fori_loop(0, w_buf.shape[1] // 512, project_block, 0)

        def step(i, _):
            rows = pl.ds(pl.multiple_of(i * 32, 32), 32)
            all_rows = pl.ds(pl.multiple_of(p * SPLIT + i * 32, 32), 32)
            attn = a_buf[rows, :].astype(jnp.bfloat16).astype(jnp.float32)
            mid = (resid_ref[all_rows, :].astype(jnp.float32) + norm_rows(attn, post_ref[...])).astype(jnp.bfloat16)
            mid_ref[all_rows, :] = mid
            h_buf[all_rows, :] = norm_rows(mid.astype(jnp.float32), next_ref[...]).astype(jnp.bfloat16)
            return 0

        lax.fori_loop(0, SPLIT // 32, step, 0)
        gather.start(p)
    for copy in moves:
        copy.wait_send()
    gather.finish()


def out_project(o_loc, out_a, out_b, resid, post, nxt, layer):
    rows, width = resid.shape
    n_tok, dim = o_loc.shape
    hbm = pl.BlockSpec(memory_space=pl.ANY)
    vmem = pl.BlockSpec(memory_space=pltpu.VMEM)
    return pl.pallas_call(
        out_kernel,
        in_specs=[hbm] * 11 + [vmem] * 3,
        out_specs=[vmem, hbm],
        out_shape=[jax.ShapeDtypeStruct((rows, width), jnp.bfloat16), jax.ShapeDtypeStruct((n_tok, width), jnp.bfloat16)],
        scratch_shapes=[pltpu.VMEM((rows, 4 * dim), jnp.bfloat16), pltpu.VMEM((4 * dim, width), jnp.bfloat16), pltpu.VMEM((SPLIT, width), jnp.float32),
                        pltpu.VMEM((rows, width), jnp.bfloat16), pltpu.SemaphoreType.DMA((5, 4)), pltpu.SemaphoreType.DMA,
                        pltpu.SemaphoreType.DMA((4,)), pltpu.SemaphoreType.DMA((4,))] + GATHER_SEMS,
        compiler_params=pltpu.CompilerParams(collective_id=3 + layer, has_side_effects=True),
        cost_estimate=pl.CostEstimate(flops=20_000_000_000, bytes_accessed=20_000_000, transcendentals=0),
    )(o_loc, *out_a, *out_b, resid, post, nxt)


FFN_ROWS = 256
FFN_COLS = 512


def ffn_kernel(make_next, h_ref, g0, g1, g2, g3, u0, u1, u2, u3, d0, d1, d2, d3, mid_ref, post_ref, next_ref, hidden_ref, full_ref,
               wg, wu, wd, h_buf, m_buf, send, own, recv, load_sem, wd_sem, h_sem, io_sem, send_sem, recv_sem, *gather_sems):
    head, over_y, over_z, diag = head_peers()
    peers = [{'heads': over_y}, {'heads': over_z}]
    if not make_next:
        me = lax.axis_index('model')
        near = me + 1 - 2 * (me % 2)
        far = me + 2 - 4 * (me // 2)
        cross = near + 2 - 4 * (me // 2)
        model_order = (me, near, far, cross)
        peers += [{'model': peer} for peer in model_order[1:]]
    chunks = (diag, over_y, over_z, head)
    depth = g0.shape[0]
    width = wg.shape[0]
    half = width // 2
    n_blocks = width // FFN_COLS

    def load_h(c):
        rows = pl.ds(pl.multiple_of(chunks[c] * FFN_ROWS, FFN_ROWS), FFN_ROWS)
        return pltpu.make_async_copy(h_ref.at[rows, :], h_buf.at[c % 2], h_sem.at[c % 2])

    def load_up(n):
        copies = []
        for j, (g, u) in enumerate(((g0, u0), (g1, u1), (g2, u2), (g3, u3))):
            cols = pl.ds(n * FFN_COLS, FFN_COLS)
            rows = pl.ds(j * depth, depth)
            copies.append(pltpu.make_async_copy(g.at[:, cols], wg.at[rows, cols], load_sem.at[n, j]))
            copies.append(pltpu.make_async_copy(u.at[:, cols], wu.at[rows, cols], load_sem.at[n, 4 + j]))
        return copies

    load_h(0).start()
    for n in range(n_blocks):
        for copy in load_up(n):
            copy.start()
    down = [pltpu.make_async_copy(d, wd.at[:, pl.ds(j * depth, depth)], wd_sem.at[j]) for j, d in enumerate((d0, d1, d2, d3))]
    for copy in down:
        copy.start()

    meet(peers)

    def up_block(c, cols):
        h = h_buf[c % 2]
        gate = jnp.dot(h, wg[:, cols], preferred_element_type=jnp.float32).astype(jnp.bfloat16).astype(jnp.float32)
        up = jnp.dot(h, wu[:, cols], preferred_element_type=jnp.float32).astype(jnp.bfloat16).astype(jnp.float32)
        m_buf[:, cols] = (jax.nn.gelu(gate, approximate=True) * up).astype(jnp.bfloat16)

    def up_chunk(c):
        load_h(c).wait()
        if c < 3:
            load_h(c + 1).start()
        if c == 0:
            for n in range(n_blocks):
                for copy in load_up(n):
                    copy.wait()
                up_block(c, slice(n * FFN_COLS, (n + 1) * FFN_COLS))
        else:
            def step(n, _):
                up_block(c, pl.ds(pl.multiple_of(n * FFN_COLS, FFN_COLS), FFN_COLS))
                return 0

            lax.fori_loop(0, n_blocks, step, 0)

    def down_half(dst, side):
        def step(n, _):
            cols = pl.ds(pl.multiple_of(n * 256, 256), 256)
            wcols = pl.ds(pl.multiple_of(side * half + n * 256, 256), 256)
            dst[:, cols] = jnp.dot(m_buf[...], wd[:, wcols], preferred_element_type=jnp.float32)
            return 0

        lax.fori_loop(0, half // 256, step, 0)

    def move(k, peer):
        return pltpu.make_async_remote_copy(src_ref=send.at[k], dst_ref=recv.at[k], send_sem=send_sem.at[k], recv_sem=recv_sem.at[k],
                                            device_id={'heads': peer}, device_id_type=pl.DeviceIdType.MESH)

    def add_received(k, got):
        def step(i, _):
            rows = pl.ds(pl.multiple_of(i * 32, 32), 32)
            send[k, rows, :] = send[k, rows, :] + recv[got, rows, :]
            return 0

        lax.fori_loop(0, FFN_ROWS // 32, step, 0)

    sends = [move(0, over_y), move(1, over_z), move(2, over_y), move(3, over_z), move(4, over_z), move(5, over_y)]
    up_chunk(0)
    for copy in down:
        copy.wait()
    down_half(send.at[0], 0)
    sends[0].start()
    down_half(send.at[1], 1)
    sends[1].start()
    up_chunk(1)
    down_half(send.at[2], 0)
    sends[2].start()
    down_half(send.at[5], 1)
    up_chunk(2)
    down_half(send.at[3], 1)
    sends[3].start()
    down_half(send.at[4], 0)
    sends[0].wait_recv()
    add_received(4, 0)
    sends[4].start()
    sends[1].wait_recv()
    add_received(5, 1)
    sends[5].start()
    up_chunk(3)
    mid_load = pltpu.make_async_copy(mid_ref, h_buf.at[0], io_sem.at[0])
    mid_load.start()
    down_half(own.at[0], 0)
    down_half(own.at[1], 1)
    mid_load.wait()
    for k in range(2, 6):
        sends[k].wait_recv()

    def finish(i, _):
        rows = pl.ds(pl.multiple_of(i * 32, 32), 32)
        a = own[0, rows, :] + recv[2, rows, :] + recv[4, rows, :]
        b = own[1, rows, :] + recv[3, rows, :] + recv[5, rows, :]
        ffn = jnp.concatenate([a, b], axis=1).astype(jnp.bfloat16).astype(jnp.float32)
        hidden = (h_buf[0, rows, :].astype(jnp.float32) + norm_rows(ffn, post_ref[...])).astype(jnp.bfloat16)
        m_buf[rows, :] = hidden
        if make_next:
            h_buf[1, rows, :] = norm_rows(hidden.astype(jnp.float32), next_ref[...]).astype(jnp.bfloat16)
        return 0

    if make_next:
        gather = HeadGather(h_buf.at[1], full_ref, *gather_sems)
        for p in range(2):
            lax.fori_loop(p * SPLIT // 32, (p + 1) * SPLIT // 32, finish, 0)
            gather.start(p)
        store = pltpu.make_async_copy(m_buf, hidden_ref, io_sem.at[1])
        store.start()
        for k in range(6):
            sends[k].wait_send()
        gather.finish()
        store.wait()
    else:
        lax.fori_loop(0, FFN_ROWS // 32, finish, 0)
        spread(m_buf, hidden_ref, model_order, io_sem.at[1], *gather_sems)
        for k in range(6):
            sends[k].wait_send()


def spread(src, out_ref, model_order, local_sem, model_send, model_recv, send_sem, recv_sem):
    head, over_y, over_z, _ = head_peers()
    part = out_ref.shape[1]
    me = model_order[0]
    rows_m = out_ref.shape[0] // 4

    def block(owner, h):
        return out_ref.at[pl.ds(pl.multiple_of(owner * rows_m + h * FFN_ROWS, FFN_ROWS), FFN_ROWS), :]

    def half(owner, h, p):
        return out_ref.at[token_rows(h, p, owner * rows_m), :]

    def to_head(a, b, j, k, peer):
        return pltpu.make_async_remote_copy(src_ref=a, dst_ref=b, send_sem=send_sem.at[j, k], recv_sem=recv_sem.at[j, k],
                                            device_id={'heads': peer}, device_id_type=MESH)

    local = pltpu.make_async_copy(src.at[:, pl.ds(0, part)], block(me, head), local_sem)
    local.start()
    across = {j: pltpu.make_async_remote_copy(src_ref=src.at[:, pl.ds(j * part, part)], dst_ref=block(me, head), send_sem=model_send.at[j],
                                              recv_sem=model_recv.at[j], device_id={'model': model_order[j]}, device_id_type=MESH) for j in (1, 2, 3)}
    for copy in across.values():
        copy.start()
    first = []
    for j, owner in enumerate(model_order):
        if j:
            across[j].wait_recv()
        here = block(owner, head)
        source = here if j else src.at[:, pl.ds(0, part)]
        first.append((to_head(source, here, j, 0, over_y), to_head(source, here, j, 1, over_z)))
        for copy in first[j]:
            copy.start()
    second = []
    for j, owner in enumerate(model_order):
        first[j][0].wait_recv()
        second.append(to_head(half(owner, over_y, 0), half(owner, over_y, 0), j, 2, over_z))
        second[-1].start()
        first[j][1].wait_recv()
        second.append(to_head(half(owner, over_z, 1), half(owner, over_z, 1), j, 3, over_y))
        second[-1].start()
    for copy in second:
        copy.wait_recv()
    for copy in second + [c for pair in first for c in pair] + list(across.values()):
        copy.wait_send()
    local.wait()


def ffn_last_kernel(*refs):
    ffn_kernel(False, *refs[:17], None, *refs[17:])


def ffn(h_full, gates, ups, downs, mid, post, nxt, layer):
    n_tok, width = h_full.shape
    rows = mid.shape[0]
    hbm = pl.BlockSpec(memory_space=pl.ANY)
    vmem = pl.BlockSpec(memory_space=pltpu.VMEM)
    if layer == 0:
        outs = [jax.ShapeDtypeStruct((rows, width), jnp.bfloat16), jax.ShapeDtypeStruct((n_tok, width), jnp.bfloat16)]
        sems = GATHER_SEMS
    else:
        outs = [jax.ShapeDtypeStruct((4 * n_tok, width // 4), jnp.bfloat16)]
        sems = [pltpu.SemaphoreType.DMA((4,)), pltpu.SemaphoreType.DMA((4,)), pltpu.SemaphoreType.DMA((4, 4)), pltpu.SemaphoreType.DMA((4, 4))]
    return pl.pallas_call(
        functools.partial(ffn_kernel, True) if layer == 0 else ffn_last_kernel,
        in_specs=[hbm] * 14 + [vmem] * 2,
        out_specs=[hbm] * len(outs),
        out_shape=outs,
        scratch_shapes=[pltpu.VMEM((width, width), jnp.bfloat16)] * 3
        + [pltpu.VMEM((2, FFN_ROWS, width), jnp.bfloat16), pltpu.VMEM((FFN_ROWS, width), jnp.bfloat16),
           pltpu.VMEM((6, FFN_ROWS, width // 2), jnp.float32), pltpu.VMEM((2, FFN_ROWS, width // 2), jnp.float32),
           pltpu.VMEM((6, FFN_ROWS, width // 2), jnp.float32),
           pltpu.SemaphoreType.DMA((width // FFN_COLS, 8)), pltpu.SemaphoreType.DMA((4,)), pltpu.SemaphoreType.DMA((2,)),
           pltpu.SemaphoreType.DMA((3,)), pltpu.SemaphoreType.DMA((6,)), pltpu.SemaphoreType.DMA((6,))] + sems,
        compiler_params=pltpu.CompilerParams(collective_id=layer, has_side_effects=True, vmem_limit_bytes=67043328),
        cost_estimate=pl.CostEstimate(flops=6 * n_tok * width * width, bytes_accessed=50_000_000, transcendentals=n_tok * width),
    )(h_full, *gates, *ups, *downs, mid, post, nxt)


def solution(mesh):
    col_spec = P(None, 'model', 'heads')
    row_spec = P(None, 'heads', 'model')
    cache_spec = P(None, None, 'heads', None)

    def swap(value, bits, axis='model'):
        return lax.ppermute(value, axis, [(i, i ^ bits) for i in range(4)])

    def gather_pieces(own):
        far = swap(own, 2)
        near = swap(own, 1)
        diag = swap(far, 1)
        return (own, near, far, diag)

    def gather_out(own):
        both = jnp.concatenate([own, swap(own, 2)], axis=-1)
        y = swap(both, 1, 'heads')
        z = swap(both, 2, 'heads')
        half = both.shape[0] // 2
        d0 = swap(y[:half], 2, 'heads')
        d1 = swap(z[half:], 1, 'heads')
        a = (both, y, z, d0, d1)
        b = tuple(swap(v, 1) for v in a)
        return a, b

    def layers(hidden_in, seg_ids, positions, w_query, w_key, w_value, w_out, w_gate, w_up, w_down, norm_scales, qk_scales):
        n_tok, part = hidden_in.shape
        me = lax.axis_index('model')
        head = lax.axis_index('heads')
        rows_m = n_tok // 4
        rows_own = n_tok // 16

        scales = jnp.concatenate([norm_scales] + [swap(norm_scales, j) for j in range(1, 4)], axis=-1)
        row = lambda l, i: scales[l, i:i + 1]

        xs = [lax.dynamic_slice(hidden_in, ((me ^ j) * rows_m + head * rows_own, 0), (rows_own, part)) for j in range(4)]
        xs = [xs[0]] + [swap(xs[j], j) for j in range(1, 4)]

        index = jnp.arange(n_tok, dtype=jnp.int32)
        starts = index - positions
        pos_loc = lax.dynamic_slice(positions, (me * rows_m,), (rows_m,))

        w_qkv = jnp.concatenate([w_query, w_key, w_value], axis=-1)
        pieces = []
        for l in range(2):
            pieces.append((gather_pieces(w_qkv[l]), gather_out(w_out[l]),
                           gather_pieces(w_gate[l]), gather_pieces(w_up[l]), gather_pieces(w_down[l])))

        hidden, h_full = first_norm(xs, row(0, 0))

        settings = ((GLOBAL_BASE, GLOBAL_FACTOR, n_tok), (LOCAL_BASE, 1.0, WINDOW))
        piece_rows = jnp.stack([(me ^ j) * rows_m for j in range(4)]).astype(jnp.int32)
        tables = []
        for rope_base, pos_factor, window in settings:
            low = lax.dynamic_slice(jnp.maximum(starts, index - (window - 1)), (me * rows_m,), (rows_m,))
            bounds = jnp.concatenate([piece_rows[:1], low[::Q_ROWS], piece_rows])
            tables.append((*rope_tables(pos_loc, HEAD_DIM, rope_base, pos_factor), low[:, None], bounds))
        caches = ()
        for l in range(2):
            qkv_p, (out_a, out_b), gate_p, up_p, down_p = pieces[l]
            cos_tab, sin_tab, low, bounds = tables[l]
            kv_loc = project(kv_kernel, h_full, qkv_p, 1, cos_tab, sin_tab, qk_scales[l, 1:2])
            kv_pieces = gather_pieces(kv_loc)
            q_loc = project(q_kernel, h_full, qkv_p, 0, cos_tab, sin_tab, qk_scales[l, 0:1])
            o_loc, *caches = attend(q_loc, kv_pieces, low, bounds, caches, l)
            if l == 0:
                o_loc, tables[1] = lax.optimization_barrier((o_loc, tables[1]))
            mid, h2_full = out_project(o_loc, out_a, out_b, hidden, row(l, 1), row(l, 2), l)
            outs = ffn(h2_full, gate_p, up_p, down_p, mid, row(l, 3), row(1, 0), l)
            if l == 0:
                hidden, h_full = outs

        return outs[0], caches[0][:, :, None, :], caches[1][:, :, None, :]

    return jax.shard_map(layers, mesh=mesh,
                         in_specs=(P(None, 'model'), P(), P(), col_spec, col_spec, col_spec, row_spec, col_spec, col_spec, row_spec, P(None, None, 'model'), P()),
                         out_specs=(P(None, 'model'), cache_spec, cache_spec),
                         check_vma=False)
```
